32 devices in a mesh: rows: 32 (over z, y, x, core).
Axes of the slice: x: 2, y: 2, z: 4, core: 2. Of those that a mesh axis runs over, the one named last changes fastest.
Arguments:
- adj_diag: int32 [512, 512], P('rows'), may hold values from -2147483648 to 2147483647
- adj_right: int32 [512, 512], P('rows'), may hold values from -2147483648 to 2147483647
- alive_diag: int32 [512, 512], P('rows'), may hold values from -2147483648 to 2147483647
- alive_right: int32 [512, 512], P('rows'), may hold values from -2147483648 to 2147483647
- truss_k: int32 [1], replicated, may hold values from 130 to 193
Outputs:
- support_field: float32 [16384, 1024], P('rows')
- removed_counts: int32 [3], replicated
The draws below stay inside these ranges and needn't reach their ends.
All inputs are finite; a program needn't handle non-finite values.
Results may differ from the reference program's by a relative error of at most 0.0003.
Values may be sent and summed in bfloat16 or wider, within the bound.
A program may use at most 64 MiB of HBM per device.

```python
import jax
import jax.numpy as jnp
from jax import lax

TILE = 512
ITERS = 3
NVERT = 16384


def vertex_levels(key, block):
    base_key = jax.random.fold_in(jax.random.fold_in(key, 7001), block)
    size_key, order_key, level_key = jax.random.split(base_key, 3)
    core_count = jax.random.randint(size_key, (), TILE // 4, 3 * TILE // 8 + 1, dtype=jnp.int32)
    order = jax.random.permutation(order_key, TILE)
    is_core = order < core_count
    levels = jax.random.randint(level_key, (TILE,), 2, 16, dtype=jnp.int32)
    return (jnp.where(is_core, jnp.int32(16), levels), is_core)


def pack_bits(tile_bits):
    shifts = jnp.arange(32, dtype=jnp.int32)
    sectioned = tile_bits.reshape(TILE // 32, 32, TILE)
    return jnp.sum(sectioned << shifts[None, :, None], axis=1, dtype=jnp.int32)


def draw_bits(key, salt, offset, alive_kind):
    blocks = NVERT // TILE

    def one_block(block):
        row_levels, row_core = vertex_levels(key, block)
        col_levels, col_core = vertex_levels(key, (block + offset) % blocks)
        edge_key = jax.random.fold_in(jax.random.fold_in(key, salt), block)
        if alive_kind:
            chance = jax.random.randint(edge_key, (TILE, TILE), 0, 8, dtype=jnp.int32)
            both_core = row_core[:, None] & col_core[None, :]
            tile_bits = jnp.where(both_core, jnp.int32(1), (chance < 7).astype(jnp.int32))
        else:
            chance = jax.random.randint(edge_key, (TILE, TILE), 0, 256, dtype=jnp.int32)
            tile_bits = (chance < row_levels[:, None] * col_levels[None, :]).astype(jnp.int32)
        return pack_bits(tile_bits)
    packed = lax.map(one_block, jnp.arange(blocks, dtype=jnp.int32))
    return packed.reshape(NVERT // 32, TILE)


def draw_adj_diag(key, part):
    return draw_bits(key, 101, 0, False)


def draw_adj_right(key, part):
    return draw_bits(key, 102, 1, False)


def draw_alive_diag(key, part):
    return draw_bits(key, 103, 0, True)


def draw_alive_right(key, part):
    return draw_bits(key, 104, 1, True)


def setup_inputs(seed: int = 0) -> dict:
    seeds = jax.random.split(jax.random.key(seed), 6)
    adj_diag = draw_adj_diag(jax.random.fold_in(seeds[5], 71), 0)
    adj_right = draw_adj_right(jax.random.fold_in(seeds[5], 71), 0)
    alive_diag = draw_alive_diag(jax.random.fold_in(seeds[5], 71), 0)
    alive_right = draw_alive_right(jax.random.fold_in(seeds[5], 71), 0)
    truss_k = jax.random.randint(seeds[4], (1,), TILE // 4 + 2, 3 * TILE // 8 + 2).astype(jnp.int32)
    return {"adj_diag": adj_diag, "adj_right": adj_right, "alive_diag": alive_diag, "alive_right": alive_right, "truss_k": truss_k}


def unpack_tiles(packed, blocks, tile):
    shifts = jnp.arange(32, dtype=jnp.int32)
    sectioned = packed.reshape(blocks, tile // 32, tile)
    tile_bits = (sectioned[:, :, None, :] >> shifts[None, None, :, None]) & 1
    return tile_bits.reshape(blocks, tile, tile)


def tile_support(pieces):
    within, across, prev_across, next_within = pieces
    inside = lax.dot_general(prev_across, prev_across, (((0,), (0,)), ((), ())), preferred_element_type=jnp.float32)
    inside = inside + jnp.dot(within, within, preferred_element_type=jnp.float32)
    inside = inside + lax.dot_general(across, across, (((1,), (1,)), ((), ())), preferred_element_type=jnp.float32)
    between = jnp.dot(within, across, preferred_element_type=jnp.float32)
    between = between + jnp.dot(across, next_within, preferred_element_type=jnp.float32)
    return inside, between


def reference(adj_diag, adj_right, alive_diag, alive_right, truss_k):
    blocks = NVERT // TILE
    upper_half = jnp.triu(unpack_tiles(adj_diag & alive_diag, blocks, TILE), 1)
    within = (upper_half + jnp.swapaxes(upper_half, 1, 2)).astype(jnp.bfloat16)
    across = unpack_tiles(adj_right & alive_right, blocks, TILE).astype(jnp.bfloat16)
    thresh = (truss_k[0] - 2).astype(jnp.float32)
    counts = []
    for step in range(ITERS):
        prev_across = jnp.roll(across, 1, axis=0)
        next_within = jnp.roll(within, -1, axis=0)
        inside, between = lax.map(tile_support, (within, across, prev_across, next_within))
        new_within = jnp.where(inside >= thresh, within, jnp.zeros_like(within))
        new_across = jnp.where(between >= thresh, across, jnp.zeros_like(across))
        lost_within = jnp.sum((within - new_within).astype(jnp.int32)) // 2
        lost_across = jnp.sum((across - new_across).astype(jnp.int32))
        counts.append(lost_within + lost_across)
        within, across = new_within, new_across
    support = jnp.concatenate([inside * within.astype(jnp.float32), between * across.astype(jnp.float32)], axis=2)
    return support.reshape(NVERT, 2 * TILE), jnp.stack(counts).astype(jnp.int32)
```

```python
import functools

import jax
import jax.numpy as jnp
from jax import lax
from jax.experimental import pallas as pl
from jax.experimental.pallas import tpu as pltpu
from jax.sharding import PartitionSpec as P

F8 = jnp.float8_e4m3fn
F32 = jnp.float32
WORD = 32
ITERS = 3


def dot_nt(lhs, rhs):
    return lax.dot_general(lhs, rhs, (((1,), (1,)), ((), ())), preferred_element_type=F32)


def send(src, dst, send_sem, recv_sem, target):
    return pltpu.make_async_remote_copy(
        src_ref=src,
        dst_ref=dst,
        send_sem=send_sem,
        recv_sem=recv_sem,
        device_id=(target,),
        device_id_type=pl.DeviceIdType.MESH,
    )


def kernel(
    n, k_ref, ad_ref, ar_ref, ld_ref, lr_ref, out_ref, cnt_ref,
    k_smem, raw, own, halo, hop, x, eye, tri, spare, psum_in, psum_next, psum_btw, psum_top, psum_far,
    mine, gathered,
    k_sem, raw_sems, send_sems, recv_sems, relay_sems, hop_send, hop_recv, cnt_send, cnt_recv, all_in,
):
    t = ad_ref.shape[1]
    words = ad_ref.shape[0]
    me = lax.axis_index("rows")
    even = lax.rem(me, 2) == 0
    barrier = pltpu.get_barrier_semaphore()

    odd = jnp.logical_not(even)
    last, mid, mid_next, root = n - 1, n // 2, n // 2 + 1, n // 2 - 1

    def greet(target):
        pl.semaphore_signal(
            barrier, inc=1, device_id=(target,), device_id_type=pl.DeviceIdType.MESH
        )

    def at(by):
        return lax.rem(me + by + n, n)

    greet(at(-1))

    @pl.when(me != last)
    def _():
        greet(at(1))

    @pl.when(even)
    def _():
        greet(at(-2))

    @pl.when(jnp.logical_and(odd, me != last))
    def _():
        greet(at(2))

    @pl.when(me == last)
    def _():
        greet(mid)
        greet(mid_next)

    @pl.when(me == mid)
    def _():
        greet(1)

    @pl.when(me == mid_next)
    def _():
        greet(0)

    @pl.when(jnp.logical_or(me < root - 2, me > root + 1))
    def _():
        greet(root)

    loads = [
        pltpu.make_async_copy(src, raw.at[i], raw_sems.at[i])
        for i, src in enumerate((ad_ref, ar_ref, ld_ref, lr_ref))
    ]
    for load in loads:
        load.start()
    k_load = pltpu.make_async_copy(k_ref, k_smem, k_sem)
    k_load.start()
    for load in loads:
        load.wait()
    own[0] = raw[0] & raw[2]
    own[1] = raw[1] & raw[3]

    AT, W, A = (pl.ds(i * t, t) for i in range(3))
    shift = lax.broadcasted_iota(jnp.int32, (WORD, t), 0)
    col = lax.broadcasted_iota(jnp.int32, (WORD, t), 1)

    half = t // 2

    def unpack(src, upper):
        for w in range(words):
            left = half if upper and 2 * w >= words else 0
            bits = (jnp.broadcast_to(src[w : w + 1, left:], (WORD, t - left)) >> shift[:, left:]) & 1
            if upper:
                bits = jnp.where(col[:, left:] - shift[:, left:] > WORD * w, bits, 0)
            yield pl.ds(WORD * w, WORD), pl.ds(left, t - left), bits.astype(F32).astype(F8)

    def put_across(src, j):
        for rows, _, bits in unpack(src, False):
            x[j, rows, A] = bits

    def put_transposed(j):
        x[j + 1, :, AT] = dot_nt(eye[...], x[j, :, A]).astype(F8)

    def put_within(src, j):
        for rows, cols, bits in unpack(src, True):
            tri[rows, cols] = bits
        flipped = dot_nt(eye[...], tri[...])
        x[j, :, W] = (flipped + tri[...].astype(F32)).astype(F8)

    row_id = lax.broadcasted_iota(jnp.int32, (t, t), 0)
    col_id = lax.broadcasted_iota(jnp.int32, (t, t), 1)
    eye[...] = jnp.where(row_id == col_id, 1.0, 0.0).astype(F32).astype(F8)
    tri[half:, :half] = jnp.zeros((t - half, half), F32).astype(F8)

    middle = jnp.logical_or(me == mid, me == mid_next)

    @pl.when(middle)
    def _():
        pl.semaphore_wait(barrier, 4)

    @pl.when(me == root)
    def _():
        pl.semaphore_wait(barrier, n - 1)

    @pl.when(jnp.logical_not(jnp.logical_or(middle, me == root)))
    def _():
        pl.semaphore_wait(barrier, 3)

    top, low = pl.ds(0, words // 2), pl.ds(words // 2, words // 2)
    whole, right = pl.ds(0, t), pl.ds(half, half)

    def pieces(source, dest, upper, sends, recvs, target):
        parts = [(top, whole), (low, right if upper else whole)]
        return [
            send(
                source.at[rows, cols], dest.at[rows, cols], sends.at[i], recvs[i], target
            )
            for i, (rows, cols) in enumerate(parts)
        ]

    def to_halo(source, slot, sends, target):
        recvs = [recv_sems.at[2 * slot + i] for i in range(2)]
        return pieces(source, halo.at[slot], slot in (1, 3, 5), sends, recvs, target)

    def to_hop(what, place, slot, target):
        recvs = [hop_recv.at[place, i] for i in range(2)]
        return pieces(own.at[what], hop.at[place], slot in (3, 5), send_sems.at[slot], recvs, target)

    def start(pieces):
        for piece in pieces:
            piece.start()

    def arrive(pieces):
        for piece in pieces:
            piece.wait_recv()

    def left(pieces):
        for piece in pieces:
            piece.wait_send()

    routes = {2: (1, 1), 3: (0, -1), 1: (0, 1), 4: (1, -1), 0: (1, 2), 5: (0, -2)}
    copies = {
        slot: to_halo(own.at[what], slot, send_sems.at[slot], at(by))
        for slot, (what, by) in routes.items()
    }
    to_right = to_halo(halo.at[2], 0, relay_sems, at(1))
    to_left = to_halo(halo.at[3], 5, relay_sems, at(-1))
    hop_in = {3: to_hop(0, 0, 3, mid_next), 4: to_hop(1, 1, 4, mid_next), 5: to_hop(0, 2, 5, mid)}
    hop_out = {
        slot: to_halo(hop.at[slot - 3], slot, hop_send.at[slot - 3], last) for slot in (3, 4, 5)
    }

    def start_or_hop(slot, source):
        @pl.when(me == source)
        def _():
            start(hop_in[slot])

        @pl.when(me != source)
        def _():
            start(copies[slot])

    start_or_hop(3, 0)
    start(copies[2])

    @pl.when(even)
    def _():
        start(copies[0])

    @pl.when(odd)
    def _():
        start_or_hop(5, 1)

    start_or_hop(4, 0)
    start(copies[1])

    @pl.when(me == root)
    def _():
        def tell(d, carry):
            pl.semaphore_signal(
                all_in, inc=1, device_id=(at(d),), device_id_type=pl.DeviceIdType.MESH
            )
            return carry

        lax.fori_loop(1, n, tell, 0)

    put_across(own.at[1], 1)

    k_load.wait()
    thresh = (k_smem[0] - 2).astype(F32)

    put_within(own.at[0], 1)
    put_transposed(1)
    psum_in[...] = dot_nt(x[1, :, t:], x[1, :, t:])
    psum_next[...] = dot_nt(x[2, :, AT], x[2, :, AT])
    psum_btw[...] = dot_nt(x[1, :, W], x[2, :, AT])

    def total(values):
        lanes = jnp.sum(values, axis=0, keepdims=True)
        return sum(lanes[:, i : i + 128] for i in range(0, t, 128))

    def keep(support, j, part):
        old = x[j, :, part].astype(F32)
        return old, jnp.where(support >= thresh, old, 0.0)

    def inside(j):
        return dot_nt(x[j], x[j])

    def between(j):
        return dot_nt(x[j, :, t:], x[j + 1, :, : 2 * t])

    counts = []

    def own_count(old_w, new_w, old_a, new_a):
        counts.append(total((old_w - new_w) + 2.0 * (old_a - new_a)))

    arrive(copies[2])

    @pl.when(even)
    def _():
        start(to_right)

    put_across(halo.at[2], 0)
    put_transposed(0)
    old_w, w0 = keep(psum_in[...] + dot_nt(x[1, :, AT], x[1, :, AT]), 1, W)
    arrive(copies[1])
    put_within(halo.at[1], 0)
    _, am = keep(between(0), 0, A)

    @pl.when(me == mid_next)
    def _():
        for slot in (3, 4):
            arrive(hop_in[slot])
            start(hop_out[slot])

    @pl.when(me == mid)
    def _():
        arrive(hop_in[5])
        start(hop_out[5])

    arrive(copies[0])
    for rows, _, bits in unpack(halo.at[0], False):
        spare[rows, :] = bits
    x[0, :, AT] = dot_nt(eye[...], spare[...]).astype(F8)
    _, wm = keep(inside(0), 0, W)
    x[0, :, W] = wm.astype(F8)
    x[0, :, A] = am.astype(F8)
    x[1, :, W] = w0.astype(F8)
    put_transposed(0)
    _, am = keep(between(0), 0, A)
    psum_in[...] = dot_nt(x[1, :, : 2 * t], x[1, :, : 2 * t])
    x[0, :, A] = am.astype(F8)
    put_transposed(0)
    psum_top[...] = dot_nt(x[1, :, AT], x[1, :, AT])
    arrive(copies[3])

    @pl.when(odd)
    def _():
        start(to_left)

    put_within(halo.at[3], 2)
    old_a, a0 = keep(psum_btw[...] + dot_nt(x[1, :, A], x[2, :, W]), 1, A)
    own_count(old_w, w0, old_a, a0)
    arrive(copies[4])
    put_across(halo.at[4], 2)
    _, w1 = keep(psum_next[...] + dot_nt(x[2, :, t:], x[2, :, t:]), 2, W)
    psum_far[...] = jnp.dot(x[2, :, W], x[2, :, A], preferred_element_type=F32)
    x[1, :, A] = a0.astype(F8)
    x[2, :, W] = w1.astype(F8)
    put_transposed(1)

    old_w, w0 = keep(psum_in[...] + dot_nt(x[1, :, A], x[1, :, A]), 1, W)
    old_a, a0 = keep(between(1), 1, A)
    own_count(old_w, w0, old_a, a0)
    psum_next[...] = dot_nt(x[2, :, : 2 * t], x[2, :, : 2 * t])
    x[1, :, W] = w0.astype(F8)
    x[1, :, A] = a0.astype(F8)

    support_w = psum_top[...] + dot_nt(x[1, :, t:], x[1, :, t:])
    old_w, w0 = keep(support_w, 1, W)
    out_ref[:, :t] = support_w * w0
    lost_w = total(old_w - w0)
    psum_btw[...] = jnp.dot(x[1, :, W], x[1, :, A], preferred_element_type=F32)
    arrive(copies[5])
    put_within(halo.at[5], 3)
    _, a1 = keep(psum_far[...] + dot_nt(x[2, :, A], x[3, :, W]), 2, A)
    x[2, :, A] = a1.astype(F8)
    _, w1 = keep(psum_next[...] + dot_nt(x[2, :, A], x[2, :, A]), 2, W)
    x[2, :, W] = w1.astype(F8)
    support_a = psum_btw[...] + dot_nt(x[1, :, A], x[2, :, W])
    old_a, a0 = keep(support_a, 1, A)
    counts.append(lost_w + 2.0 * total(old_a - a0))
    lane = lax.broadcasted_iota(jnp.int32, (1, 128), 1)
    packed = jnp.zeros((1, 128), F32)
    for step, row in enumerate(counts):
        packed = jnp.where(lane == step, jnp.sum(row, axis=1, keepdims=True), packed)
    mine[...] = packed.astype(jnp.int32)

    def share(d, carry):
        send(mine, gathered.at[d - 1], cnt_send, cnt_recv, lax.rem(me + d, n)).start()
        return carry

    @pl.when(me != root)
    def _():
        pl.semaphore_wait(all_in, 1)

    lax.fori_loop(1, n, share, 0)
    out_ref[:, t:] = support_a * a0
    for slot in range(1, 5):
        left(copies[slot])

    @pl.when(even)
    def _():
        left(copies[0])
        left(to_right)

    @pl.when(odd)
    def _():
        left(copies[5])
        left(to_left)

    @pl.when(me == mid_next)
    def _():
        left(hop_out[3])
        left(hop_out[4])

    @pl.when(me == mid)
    def _():
        left(hop_out[5])

    pltpu.make_async_copy(gathered, gathered, cnt_recv).wait()
    cnt_ref[: n - 1] = gathered[...]
    cnt_ref[n - 1] = mine[...]
    pltpu.make_async_copy(gathered, gathered, cnt_send).wait()


def finish(support_ref, cnt_ref, out_ref, removed_ref, sems):
    parts = sems.shape[0]
    rows = support_ref.shape[0] // parts
    copies = [
        pltpu.make_async_copy(
            support_ref.at[pl.ds(i * rows, rows)], out_ref.at[pl.ds(i * rows, rows)], sems.at[i]
        )
        for i in range(parts)
    ]
    for copy in copies:
        copy.start()
    summed = jnp.sum(cnt_ref[...], axis=0)
    lane = lax.broadcasted_iota(jnp.int32, summed.shape, 1)
    for step in range(removed_ref.shape[0]):
        removed_ref[step] = jnp.sum(jnp.where(lane == step, summed, 0)) // 2
    for copy in copies:
        copy.wait()


def on_device(n, adj_diag, adj_right, alive_diag, alive_right, truss_k):
    words, t = adj_diag.shape
    vmem = pl.BlockSpec(memory_space=pltpu.VMEM)
    smem = pl.BlockSpec(memory_space=pltpu.SMEM)
    hbm = pl.BlockSpec(memory_space=pltpu.HBM)
    args = [
        pltpu.with_memory_space_constraint(v, pltpu.HBM)
        for v in (adj_diag, adj_right, alive_diag, alive_right)
    ]
    support, counts = pl.pallas_call(
        functools.partial(kernel, n),
        out_shape=(
            jax.ShapeDtypeStruct((t, 2 * t), F32),
            jax.ShapeDtypeStruct((n, 1, 128), jnp.int32),
        ),
        in_specs=[hbm] * 5,
        out_specs=(vmem, vmem),
        scratch_shapes=[
            pltpu.SMEM((1,), jnp.int32),
            pltpu.VMEM((4, words, t), jnp.int32),
            pltpu.VMEM((2, words, t), jnp.int32),
            pltpu.VMEM((6, words, t), jnp.int32),
            pltpu.VMEM((3, words, t), jnp.int32),
            pltpu.VMEM((4, t, 3 * t), F8),
            pltpu.VMEM((t, t), F8),
            pltpu.VMEM((t, t), F8),
            pltpu.VMEM((t, t), F8),
            pltpu.VMEM((t, t), F32),
            pltpu.VMEM((t, t), F32),
            pltpu.VMEM((t, t), F32),
            pltpu.VMEM((t, t), F32),
            pltpu.VMEM((t, t), F32),
            pltpu.VMEM((1, 128), jnp.int32),
            pltpu.VMEM((n - 1, 1, 128), jnp.int32),
            pltpu.SemaphoreType.DMA,
            pltpu.SemaphoreType.DMA((4,)),
            pltpu.SemaphoreType.DMA((6, 2)),
            pltpu.SemaphoreType.DMA((12,)),
            pltpu.SemaphoreType.DMA((2,)),
            pltpu.SemaphoreType.DMA((3, 2)),
            pltpu.SemaphoreType.DMA((3, 2)),
            pltpu.SemaphoreType.DMA,
            pltpu.SemaphoreType.DMA,
            pltpu.SemaphoreType.REGULAR,
        ],
        compiler_params=pltpu.CompilerParams(collective_id=0, has_side_effects=True, vmem_limit_bytes=24 * 2**20),
    )(truss_k, *args)
    return pl.pallas_call(
        finish,
        out_shape=(
            jax.ShapeDtypeStruct((t, 2 * t), F32),
            jax.ShapeDtypeStruct((ITERS,), jnp.int32),
        ),
        in_specs=[vmem, vmem],
        out_specs=(hbm, smem),
        scratch_shapes=[pltpu.SemaphoreType.DMA((4,))],
        compiler_params=pltpu.CompilerParams(vmem_limit_bytes=2**20),
    )(support, counts)


def solution(mesh):
    row = P("rows", None)
    return jax.shard_map(
        functools.partial(on_device, mesh.shape["rows"]),
        mesh=mesh,
        in_specs=(row, row, row, row, P()),
        out_specs=(row, P()),
        check_vma=False,
    )
```

```python
import functools

import jax
import jax.numpy as jnp
from jax import lax
from jax.experimental import pallas as pl
from jax.experimental.pallas import tpu as pltpu
from jax.sharding import PartitionSpec as P

F8 = jnp.float8_e4m3fn
F32 = jnp.float32
WORD = 32
ITERS = 3


def dot_nt(lhs, rhs):
    return lax.dot_general(lhs, rhs, (((1,), (1,)), ((), ())), preferred_element_type=F32)


def send(src, dst, send_sem, recv_sem, target):
    return pltpu.make_async_remote_copy(
        src_ref=src,
        dst_ref=dst,
        send_sem=send_sem,
        recv_sem=recv_sem,
        device_id=(target,),
        device_id_type=pl.DeviceIdType.MESH,
    )


def kernel(
    n, k_ref, ad_ref, ar_ref, ld_ref, lr_ref, out_ref, cnt_ref,
    k_smem, raw, own, halo, hop, x0, x1, x2, eye, tri, spare, sums, mine, gathered,
    part_w0, part_a0, part_w1, part_a1, part_wm, part_sw, part_sa, part_top,
    k_sem, raw_sems, send_sems, recv_sems, relay_sems, hop_send, hop_recv, cnt_send, cnt_recv,
    all_in, last_in,
):
    t = ad_ref.shape[1]
    words = ad_ref.shape[0]
    me = lax.axis_index("rows")
    even = lax.rem(me, 2) == 0
    barrier = pltpu.get_barrier_semaphore()

    odd = jnp.logical_not(even)
    last, mid, mid_next, root = n - 1, n // 2, n // 2 + 1, n - 3

    def greet(target):
        pl.semaphore_signal(
            barrier, inc=1, device_id=(target,), device_id_type=pl.DeviceIdType.MESH
        )

    def at(by):
        return lax.rem(me + by + n, n)

    greet(at(-1))

    @pl.when(me != last)
    def _():
        greet(at(1))

    @pl.when(even)
    def _():
        greet(at(-2))

    @pl.when(jnp.logical_and(odd, me != last))
    def _():
        greet(at(2))

    @pl.when(me == mid)
    def _():
        greet(1)
        greet(last)

    @pl.when(me == mid_next)
    def _():
        greet(0)
        greet(last)

    @pl.when(jnp.logical_or(me < root - 2, me == last))
    def _():
        greet(root)

    loads = [
        pltpu.make_async_copy(src, raw.at[i], raw_sems.at[i])
        for i, src in enumerate((ad_ref, ar_ref, ld_ref, lr_ref))
    ]
    for load in loads:
        load.start()
    k_load = pltpu.make_async_copy(k_ref, k_smem, k_sem)
    k_load.start()
    @pl.when(me == last)
    def _():
        pl.semaphore_wait(barrier, 5)
        for target in (mid, mid_next):
            pl.semaphore_signal(
                last_in, inc=1, device_id=(target,), device_id_type=pl.DeviceIdType.MESH
            )

    for load in loads:
        load.wait()
    own[0] = raw[0] & raw[2]
    own[1] = raw[1] & raw[3]

    AT, W, A = (pl.ds(i * t, t) for i in range(3))
    shift = lax.broadcasted_iota(jnp.int32, (WORD, t), 0)
    slope = lax.broadcasted_iota(jnp.int32, (WORD, 128), 1) - shift[:, :128]

    half = t // 2

    def bits_of(src, w, cols):
        span = cols.size
        words32 = jnp.broadcast_to(src[w : w + 1, cols], (WORD, span))
        return (words32 >> shift[:, :span]) & 1

    def put_across(src, dst):
        for w in range(words):
            dst[pl.ds(WORD * w, WORD), :] = bits_of(src, w, pl.ds(0, t)).astype(F32).astype(F8)

    halves = (pl.ds(0, half), pl.ds(half, half))

    def flipped(src, rows, cols):
        return dot_nt(eye[...], src[cols, rows])

    def put_flipped(src, dst):
        for rows in halves:
            for cols in halves:
                dst[rows, cols] = flipped(src, rows, cols).astype(F8)

    def put_within(src, dst):
        for w in range(words):
            rows, edge = pl.ds(WORD * w, WORD), WORD * w // 128 * 128
            bits = bits_of(src, w, pl.ds(edge, 128))
            bits = jnp.where(slope > WORD * w - edge, bits, 0)
            tri[rows, pl.ds(edge, 128)] = bits.astype(F32).astype(F8)
            if edge + 128 < t:
                rest = pl.ds(edge + 128, t - edge - 128)
                tri[rows, rest] = bits_of(src, w, rest).astype(F32).astype(F8)
        for rows in halves:
            both = flipped(tri, rows, rows) + tri[rows, rows].astype(F32)
            dst[rows, rows] = both.astype(F8)
        first, second = halves
        dst[first, second] = tri[first, second]
        dst[second, first] = flipped(tri, second, first).astype(F8)

    row_id = lax.broadcasted_iota(jnp.int32, (half, half), 0)
    col_id = lax.broadcasted_iota(jnp.int32, (half, half), 1)
    eye[...] = jnp.where(row_id == col_id, 1.0, 0.0).astype(F32).astype(F8)
    tri[...] = jnp.zeros((t, t), F32).astype(F8)

    @pl.when(me == root)
    def _():
        pl.semaphore_wait(barrier, n - 1)

    @pl.when(jnp.logical_and(me != root, me != last))
    def _():
        pl.semaphore_wait(barrier, 3)

    top, low = pl.ds(0, words // 2), pl.ds(words // 2, words // 2)
    whole, right = pl.ds(0, t), pl.ds(half, half)

    def pieces(source, dest, upper, sends, recvs, target):
        parts = [(top, whole), (low, right if upper else whole)]
        return [
            send(
                source.at[rows, cols], dest.at[rows, cols], sends.at[i], recvs[i], target
            )
            for i, (rows, cols) in enumerate(parts)
        ]

    def to_halo(source, slot, sends, target):
        recvs = [recv_sems.at[2 * slot + i] for i in range(2)]
        return pieces(source, halo.at[slot], slot in (1, 3, 5), sends, recvs, target)

    def to_hop(what, place, slot, target):
        recvs = [hop_recv.at[place, i] for i in range(2)]
        return pieces(own.at[what], hop.at[place], slot in (3, 5), send_sems.at[slot], recvs, target)

    def start(pieces):
        for piece in pieces:
            piece.start()

    def arrive(pieces):
        for piece in pieces:
            piece.wait_recv()

    def left(pieces):
        for piece in pieces:
            piece.wait_send()

    routes = {2: (1, 1), 3: (0, -1), 1: (0, 1), 4: (1, -1), 0: (1, 2), 5: (0, -2)}
    copies = {
        slot: to_halo(own.at[what], slot, send_sems.at[slot], at(by))
        for slot, (what, by) in routes.items()
    }
    to_right = to_halo(halo.at[2], 0, relay_sems, at(1))
    to_left = to_halo(halo.at[3], 5, relay_sems, at(-1))
    hop_in = {3: to_hop(0, 0, 3, mid_next), 4: to_hop(1, 1, 4, mid_next), 5: to_hop(0, 2, 5, mid)}
    hop_out = {
        slot: to_halo(hop.at[slot - 3], slot, hop_send.at[slot - 3], last) for slot in (3, 4, 5)
    }

    def start_or_hop(slot, source):
        @pl.when(me == source)
        def _():
            start(hop_in[slot])

        @pl.when(me != source)
        def _():
            start(copies[slot])

    start_or_hop(3, 0)
    start(copies[2])
    start_or_hop(4, 0)
    start(copies[1])

    @pl.when(me == 1)
    def _():
        start(hop_in[5])

    @pl.when(me == root)
    def _():
        def tell(d, carry):
            pl.semaphore_signal(
                all_in, inc=1, device_id=(at(d),), device_id_type=pl.DeviceIdType.MESH
            )
            return carry

        lax.fori_loop(1, n, tell, 0)

    def total(values):
        lanes = jnp.sum(values, axis=0, keepdims=True)
        return sum(lanes[:, i : i + 128] for i in range(0, t, 128))

    def keep(support, ref):
        old = ref.astype(F32)
        return old, jnp.where(support >= thresh, old, 0.0)

    def put_sum(row, values):
        sums[row : row + 1, :] = total(values)

    def plain(lhs, rhs):
        return jnp.dot(lhs, rhs, preferred_element_type=F32)

    def square(block):
        return dot_nt(block, block)

    def between(x, j):
        return dot_nt(x[j, :, t:], x[j + 1, :, : 2 * t])

    put_across(own.at[1], x0.at[1, :, A])
    k_load.wait()
    thresh = (k_smem[0] - 2).astype(F32)
    put_within(own.at[0], x0.at[1, :, W])
    put_flipped(x0.at[1, :, A], x0.at[2, :, AT])
    part_w0[...] = square(x0[1, :, t:])
    part_w1[...] = square(x0[2, :, AT])
    part_a0[...] = dot_nt(x0[1, :, W], x0[2, :, AT])

    @pl.when(even)
    def _():
        start(copies[0])

    @pl.when(jnp.logical_and(odd, me != 1))
    def _():
        start(copies[5])

    def left_near():
        arrive(copies[2])

        @pl.when(even)
        def _():
            start(to_right)

        arrive(copies[1])
        put_across(halo.at[2], x0.at[0, :, A])
        put_flipped(x0.at[0, :, A], x0.at[1, :, AT])
        old, new = keep(part_w0[...] + square(x0[1, :, AT]), x0[1, :, W])
        put_sum(0, old)
        put_sum(2, new)
        x1[1, :, W] = new.astype(F8)
        put_within(halo.at[1], x0.at[0, :, W])
        _, new = keep(between(x0, 0), x0[0, :, A])
        x1[0, :, A] = new.astype(F8)
        put_flipped(x1.at[0, :, A], x1.at[1, :, AT])
        part_wm[...] = square(x0[0, :, t:])
        part_w0[...] = square(x1[1, :, : 2 * t])

    def left_far():
        put_across(halo.at[0], spare)
        put_flipped(spare, x0.at[0, :, AT])
        _, new = keep(part_wm[...] + square(x0[0, :, AT]), x0[0, :, W])
        x1[0, :, W] = new.astype(F8)
        _, new = keep(between(x1, 0), x1[0, :, A])
        spare[...] = new.astype(F8)
        put_flipped(spare, x2.at[0, :, AT])
        part_top[...] = square(x2[0, :, AT])

    def right_near():
        arrive(copies[3])

        @pl.when(odd)
        def _():
            start(to_left)

        arrive(copies[4])
        put_within(halo.at[3], x0.at[2, :, W])
        old, new = keep(part_a0[...] + dot_nt(x0[1, :, A], x0[2, :, W]), x0[1, :, A])
        put_sum(1, old)
        put_sum(3, new)
        x1[1, :, A] = new.astype(F8)
        put_flipped(x1.at[1, :, A], x1.at[2, :, AT])
        put_across(halo.at[4], x0.at[2, :, A])
        _, new = keep(part_w1[...] + square(x0[2, :, t:]), x0[2, :, W])
        x1[2, :, W] = new.astype(F8)
        part_a1[...] = plain(x0[2, :, W], x0[2, :, A])
        part_w1[...] = square(x1[2, :, : 2 * t])

    @pl.when(odd)
    def _():
        left_near()

    @pl.when(even)
    def _():
        right_near()

    @pl.when(me == mid)
    def _():
        pl.semaphore_wait(last_in, 1)
        arrive(hop_in[5])
        start(hop_out[5])

    @pl.when(me == mid_next)
    def _():
        pl.semaphore_wait(last_in, 1)
        for slot in (3, 4):
            arrive(hop_in[slot])
            start(hop_out[slot])

    @pl.when(me == last)
    def _():
        arrive(copies[0])
        left_far()

    @pl.when(even)
    def _():
        left_near()

    @pl.when(odd)
    def _():
        right_near()

    def finish_rounds(far):
        arrive(copies[5])
        put_within(halo.at[5], x0.at[3, :, W])
        _, new = keep(part_w0[...] + square(x1[1, :, A]), x1[1, :, W])
        put_sum(4, new)
        x2[0, :, W] = new.astype(F8)
        _, new = keep(between(x1, 1), x1[1, :, A])
        put_sum(5, new)
        x2[0, :, A] = new.astype(F8)
        _, new = keep(part_a1[...] + dot_nt(x0[2, :, A], x0[3, :, W]), x0[2, :, A])
        x1[2, :, A] = new.astype(F8)
        part_sw[...] = square(x2[0, :, t:])
        if far:
            left_far()
        _, new = keep(part_w1[...] + square(x1[2, :, A]), x1[2, :, W])
        x2[1, :, W] = new.astype(F8)
        part_sa[...] = plain(x2[0, :, W], x2[0, :, A])
        support = part_sw[...] + part_top[...]
        _, new = keep(support, x2[0, :, W])
        put_sum(6, new)
        out_ref[:, :t] = support * new
        support = part_sa[...] + dot_nt(x2[0, :, A], x2[1, :, W])
        _, new = keep(support, x2[0, :, A])
        put_sum(7, new)
        out_ref[:, t:] = support * new

    @pl.when(me == last)
    def _():
        finish_rounds(False)

    @pl.when(me != last)
    def _():
        arrive(copies[0])
        finish_rounds(True)

    counts = []
    for step in range(ITERS):
        before, after = sums[2 * step : 2 * step + 2, :], sums[2 * step + 2 : 2 * step + 4, :]
        gone = before - after
        counts.append(gone[0:1] + 2.0 * gone[1:2])
    lane = lax.broadcasted_iota(jnp.int32, (1, 128), 1)
    packed = jnp.zeros((1, 128), F32)
    for step, row in enumerate(counts):
        packed = jnp.where(lane == step, jnp.sum(row, axis=1, keepdims=True), packed)
    mine[...] = packed.astype(jnp.int32)

    def share(d, carry):
        send(mine, gathered.at[d - 1], cnt_send, cnt_recv, lax.rem(me + d, n)).start()
        return carry

    @pl.when(me != root)
    def _():
        pl.semaphore_wait(all_in, 1)

    lax.fori_loop(1, n, share, 0)
    for slot in range(1, 5):
        left(copies[slot])

    @pl.when(even)
    def _():
        left(copies[0])
        left(to_right)

    @pl.when(odd)
    def _():
        left(copies[5])
        left(to_left)

    @pl.when(me == mid_next)
    def _():
        left(hop_out[3])
        left(hop_out[4])

    @pl.when(me == mid)
    def _():
        left(hop_out[5])

    pltpu.make_async_copy(gathered, gathered, cnt_recv).wait()
    cnt_ref[: n - 1] = gathered[...]
    cnt_ref[n - 1] = mine[...]
    pltpu.make_async_copy(gathered, gathered, cnt_send).wait()


def finish(support_ref, cnt_ref, out_ref, removed_ref, sems):
    parts = sems.shape[0]
    rows = support_ref.shape[0] // parts
    copies = [
        pltpu.make_async_copy(
            support_ref.at[pl.ds(i * rows, rows)], out_ref.at[pl.ds(i * rows, rows)], sems.at[i]
        )
        for i in range(parts)
    ]
    for copy in copies:
        copy.start()
    summed = jnp.sum(cnt_ref[...], axis=0)
    lane = lax.broadcasted_iota(jnp.int32, summed.shape, 1)
    for step in range(removed_ref.shape[0]):
        removed_ref[step] = jnp.sum(jnp.where(lane == step, summed, 0)) // 2
    for copy in copies:
        copy.wait()


def on_device(n, adj_diag, adj_right, alive_diag, alive_right, truss_k):
    words, t = adj_diag.shape
    vmem = pl.BlockSpec(memory_space=pltpu.VMEM)
    smem = pl.BlockSpec(memory_space=pltpu.SMEM)
    hbm = pl.BlockSpec(memory_space=pltpu.HBM)
    args = [
        pltpu.with_memory_space_constraint(v, pltpu.HBM)
        for v in (adj_diag, adj_right, alive_diag, alive_right)
    ]
    support, counts = pl.pallas_call(
        functools.partial(kernel, n),
        out_shape=(
            jax.ShapeDtypeStruct((t, 2 * t), F32),
            jax.ShapeDtypeStruct((n, 1, 128), jnp.int32),
        ),
        in_specs=[hbm] * 5,
        out_specs=(vmem, vmem),
        scratch_shapes=[
            pltpu.SMEM((1,), jnp.int32),
            pltpu.VMEM((4, words, t), jnp.int32),
            pltpu.VMEM((2, words, t), jnp.int32),
            pltpu.VMEM((6, words, t), jnp.int32),
            pltpu.VMEM((3, words, t), jnp.int32),
            pltpu.VMEM((4, t, 3 * t), F8),
            pltpu.VMEM((3, t, 3 * t), F8),
            pltpu.VMEM((2, t, 3 * t), F8),
            pltpu.VMEM((t // 2, t // 2), F8),
            pltpu.VMEM((t, t), F8),
            pltpu.VMEM((t, t), F8),
            pltpu.VMEM((8, 128), F32),
            pltpu.VMEM((1, 128), jnp.int32),
            pltpu.VMEM((n - 1, 1, 128), jnp.int32),
            *[pltpu.VMEM((t, t), F32)] * 8,
            pltpu.SemaphoreType.DMA,
            pltpu.SemaphoreType.DMA((4,)),
            pltpu.SemaphoreType.DMA((6, 2)),
            pltpu.SemaphoreType.DMA((12,)),
            pltpu.SemaphoreType.DMA((2,)),
            pltpu.SemaphoreType.DMA((3, 2)),
            pltpu.SemaphoreType.DMA((3, 2)),
            pltpu.SemaphoreType.DMA,
            pltpu.SemaphoreType.DMA,
            pltpu.SemaphoreType.REGULAR,
            pltpu.SemaphoreType.REGULAR,
        ],
        compiler_params=pltpu.CompilerParams(collective_id=0, has_side_effects=True, vmem_limit_bytes=32 * 2**20),
    )(truss_k, *args)
    return pl.pallas_call(
        finish,
        out_shape=(
            jax.ShapeDtypeStruct((t, 2 * t), F32),
            jax.ShapeDtypeStruct((ITERS,), jnp.int32),
        ),
        in_specs=[vmem, vmem],
        out_specs=(hbm, smem),
        scratch_shapes=[pltpu.SemaphoreType.DMA((4,))],
        compiler_params=pltpu.CompilerParams(vmem_limit_bytes=2**20),
    )(support, counts)


def solution(mesh):
    row = P("rows", None)
    return jax.shard_map(
        functools.partial(on_device, mesh.shape["rows"]),
        mesh=mesh,
        in_specs=(row, row, row, row, P()),
        out_specs=(row, P()),
        check_vma=False,
    )
```

```python
import functools

import jax
import jax.numpy as jnp
from jax import lax
from jax.experimental import pallas as pl
from jax.experimental.pallas import tpu as pltpu
from jax.sharding import PartitionSpec as P

F8 = jnp.float8_e4m3fn
F32 = jnp.float32
WORD = 32
ITERS = 3


def dot_nt(lhs, rhs):
    return lax.dot_general(lhs, rhs, (((1,), (1,)), ((), ())), preferred_element_type=F32)


def send(src, dst, send_sem, recv_sem, target):
    return pltpu.make_async_remote_copy(
        src_ref=src,
        dst_ref=dst,
        send_sem=send_sem,
        recv_sem=recv_sem,
        device_id=(target,),
        device_id_type=pl.DeviceIdType.MESH,
    )


def kernel(
    n, k_ref, ad_ref, ar_ref, ld_ref, lr_ref, out_ref, cnt_ref,
    k_smem, raw, own, halo, hop, x0, x1, x2, eye, tri, spare, sums, mine, gathered,
    part_w0, part_a0, part_w1, part_top,
    k_sem, raw_sems, send_sems, recv_sems, relay_sems, hop_send, hop_recv, cnt_send, cnt_recv,
    all_in, last_in,
):
    t = ad_ref.shape[1]
    words = ad_ref.shape[0]
    me = lax.axis_index("rows")
    even = lax.rem(me, 2) == 0
    barrier = pltpu.get_barrier_semaphore()

    odd = jnp.logical_not(even)
    last, mid, mid_next, root = n - 1, n // 2, n // 2 + 1, n - 3

    def greet(target):
        pl.semaphore_signal(
            barrier, inc=1, device_id=(target,), device_id_type=pl.DeviceIdType.MESH
        )

    def at(by):
        return lax.rem(me + by + n, n)

    greet(at(-1))

    @pl.when(me != last)
    def _():
        greet(at(1))

    @pl.when(even)
    def _():
        greet(at(-2))

    @pl.when(jnp.logical_and(odd, me != last))
    def _():
        greet(at(2))

    @pl.when(me == mid)
    def _():
        greet(1)
        greet(last)

    @pl.when(me == mid_next)
    def _():
        greet(0)
        greet(last)

    @pl.when(jnp.logical_or(me < root - 2, me == last))
    def _():
        greet(root)

    loads = [
        pltpu.make_async_copy(src, raw.at[i], raw_sems.at[i])
        for i, src in enumerate((ad_ref, ar_ref, ld_ref, lr_ref))
    ]
    for load in loads:
        load.start()
    k_load = pltpu.make_async_copy(k_ref, k_smem, k_sem)
    k_load.start()
    @pl.when(me == last)
    def _():
        pl.semaphore_wait(barrier, 5)
        for target in (mid, mid_next):
            pl.semaphore_signal(
                last_in, inc=1, device_id=(target,), device_id_type=pl.DeviceIdType.MESH
            )

    for load in loads:
        load.wait()
    own[0] = raw[0] & raw[2]
    own[1] = raw[1] & raw[3]

    AT, W, A = (pl.ds(i * t, t) for i in range(3))
    shift = lax.broadcasted_iota(jnp.int32, (WORD, t), 0)
    slope = lax.broadcasted_iota(jnp.int32, (WORD, 128), 1) - shift[:, :128]

    half = t // 2

    def bits_of(src, w, cols):
        span = cols.size
        words32 = jnp.broadcast_to(src[w : w + 1, cols], (WORD, span))
        return (words32 >> shift[:, :span]) & 1

    def put_across(src, dst):
        for w in range(words):
            dst[pl.ds(WORD * w, WORD), :] = bits_of(src, w, pl.ds(0, t)).astype(F32).astype(F8)

    halves = (pl.ds(0, half), pl.ds(half, half))

    def flipped(src, rows, cols):
        return dot_nt(eye[...], src[cols, rows])

    def put_flipped(src, dst):
        for rows in halves:
            for cols in halves:
                dst[rows, cols] = flipped(src, rows, cols).astype(F8)

    def put_within(src, dst):
        for w in range(words):
            rows, edge = pl.ds(WORD * w, WORD), WORD * w // 128 * 128
            bits = bits_of(src, w, pl.ds(edge, 128))
            bits = jnp.where(slope > WORD * w - edge, bits, 0)
            tri[rows, pl.ds(edge, 128)] = bits.astype(F32).astype(F8)
            if edge + 128 < t:
                rest = pl.ds(edge + 128, t - edge - 128)
                tri[rows, rest] = bits_of(src, w, rest).astype(F32).astype(F8)
        for rows in halves:
            both = flipped(tri, rows, rows) + tri[rows, rows].astype(F32)
            dst[rows, rows] = both.astype(F8)
        first, second = halves
        dst[first, second] = tri[first, second]
        dst[second, first] = flipped(tri, second, first).astype(F8)

    row_id = lax.broadcasted_iota(jnp.int32, (half, half), 0)
    col_id = lax.broadcasted_iota(jnp.int32, (half, half), 1)
    eye[...] = jnp.where(row_id == col_id, 1.0, 0.0).astype(F32).astype(F8)
    tri[...] = jnp.zeros((t, t), F32).astype(F8)

    @pl.when(me == root)
    def _():
        pl.semaphore_wait(barrier, n - 1)

    @pl.when(jnp.logical_and(me != root, me != last))
    def _():
        pl.semaphore_wait(barrier, 3)

    top, low = pl.ds(0, words // 2), pl.ds(words // 2, words // 2)
    whole, right = pl.ds(0, t), pl.ds(half, half)

    def pieces(source, dest, upper, sends, recvs, target):
        parts = [(top, whole), (low, right if upper else whole)]
        return [
            send(
                source.at[rows, cols], dest.at[rows, cols], sends.at[i], recvs[i], target
            )
            for i, (rows, cols) in enumerate(parts)
        ]

    def to_halo(source, slot, sends, target):
        recvs = [recv_sems.at[2 * slot + i] for i in range(2)]
        return pieces(source, halo.at[slot], slot in (1, 3, 5), sends, recvs, target)

    def to_hop(what, place, slot, target):
        recvs = [hop_recv.at[place, i] for i in range(2)]
        return pieces(own.at[what], hop.at[place], slot in (3, 5), send_sems.at[slot], recvs, target)

    def start(pieces):
        for piece in pieces:
            piece.start()

    def arrive(pieces):
        for piece in pieces:
            piece.wait_recv()

    def left(pieces):
        for piece in pieces:
            piece.wait_send()

    routes = {2: (1, 1), 3: (0, -1), 1: (0, 1), 4: (1, -1), 0: (1, 2), 5: (0, -2)}
    copies = {
        slot: to_halo(own.at[what], slot, send_sems.at[slot], at(by))
        for slot, (what, by) in routes.items()
    }
    to_right = to_halo(halo.at[2], 0, relay_sems, at(1))
    to_left = to_halo(halo.at[3], 5, relay_sems, at(-1))
    hop_in = {3: to_hop(0, 0, 3, mid_next), 4: to_hop(1, 1, 4, mid_next), 5: to_hop(0, 2, 5, mid)}
    hop_out = {
        slot: to_halo(hop.at[slot - 3], slot, hop_send.at[slot - 3], last) for slot in (3, 4, 5)
    }

    def start_or_hop(slot, source):
        @pl.when(me == source)
        def _():
            start(hop_in[slot])

        @pl.when(me != source)
        def _():
            start(copies[slot])

    start_or_hop(3, 0)
    start(copies[2])
    start_or_hop(4, 0)
    start(copies[1])

    @pl.when(me == 1)
    def _():
        start(hop_in[5])

    @pl.when(me == root)
    def _():
        def tell(d, carry):
            pl.semaphore_signal(
                all_in, inc=1, device_id=(at(d),), device_id_type=pl.DeviceIdType.MESH
            )
            return carry

        lax.fori_loop(1, n, tell, 0)

    def total(values):
        lanes = jnp.sum(values, axis=0, keepdims=True)
        return sum(lanes[:, i : i + 128] for i in range(0, t, 128))

    def keep(support, ref):
        old = ref.astype(F32)
        return old, jnp.where(support >= thresh, old, 0.0)

    def put_sum(row, values):
        sums[row : row + 1, :] = total(values)

    def plain(lhs, rhs):
        return jnp.dot(lhs, rhs, preferred_element_type=F32)

    def square(block):
        return dot_nt(block, block)

    def between(x, j):
        return dot_nt(x[j, :, t:], x[j + 1, :, : 2 * t])

    put_across(own.at[1], x0.at[1, :, A])
    k_load.wait()
    thresh = (k_smem[0] - 2).astype(F32)
    put_within(own.at[0], x0.at[1, :, W])
    put_flipped(x0.at[1, :, A], x0.at[2, :, AT])
    part_w0[...] = square(x0[1, :, t:])
    part_w1[...] = square(x0[2, :, AT])
    part_a0[...] = dot_nt(x0[1, :, W], x0[2, :, AT])

    @pl.when(even)
    def _():
        start(copies[0])

    @pl.when(jnp.logical_and(odd, me != 1))
    def _():
        start(copies[5])

    def left_near():
        arrive(copies[2])

        @pl.when(even)
        def _():
            start(to_right)

        arrive(copies[1])
        put_across(halo.at[2], x0.at[0, :, A])
        put_flipped(x0.at[0, :, A], x0.at[1, :, AT])
        old, new = keep(part_w0[...] + square(x0[1, :, AT]), x0[1, :, W])
        put_sum(0, old)
        put_sum(2, new)
        x1[1, :, W] = new.astype(F8)
        put_within(halo.at[1], x0.at[0, :, W])
        _, new = keep(between(x0, 0), x0[0, :, A])
        x1[0, :, A] = new.astype(F8)
        put_flipped(x1.at[0, :, A], x1.at[1, :, AT])

    def left_far():
        put_across(halo.at[0], spare)
        put_flipped(spare, x0.at[0, :, AT])
        _, new = keep(square(x0[0]), x0[0, :, W])
        x1[0, :, W] = new.astype(F8)
        _, new = keep(between(x1, 0), x1[0, :, A])
        spare[...] = new.astype(F8)
        put_flipped(spare, x2.at[0, :, AT])

    def right_near(split):
        arrive(copies[3])

        @pl.when(odd)
        def _():
            start(to_left)

        if not split:
            arrive(copies[4])
        put_within(halo.at[3], x0.at[2, :, W])
        old, new = keep(part_a0[...] + dot_nt(x0[1, :, A], x0[2, :, W]), x0[1, :, A])
        put_sum(1, old)
        put_sum(3, new)
        x1[1, :, A] = new.astype(F8)
        put_flipped(x1.at[1, :, A], x1.at[2, :, AT])
        if split:
            arrive(copies[4])
        put_across(halo.at[4], x0.at[2, :, A])
        _, new = keep(part_w1[...] + square(x0[2, :, t:]), x0[2, :, W])
        x1[2, :, W] = new.astype(F8)

    @pl.when(me == mid_next)
    def _():
        pl.semaphore_wait(last_in, 1)
        for slot in (3, 4):
            arrive(hop_in[slot])
            start(hop_out[slot])

    @pl.when(odd)
    def _():
        left_near()

    @pl.when(even)
    def _():
        right_near(False)

    @pl.when(me == mid)
    def _():
        pl.semaphore_wait(last_in, 1)
        arrive(hop_in[5])
        start(hop_out[5])

    @pl.when(me == last)
    def _():
        arrive(copies[0])
        left_far()
        part_w0[...] = square(x1[1, :, : 2 * t])
        part_top[...] = square(x2[0, :, AT])
        right_near(True)

    @pl.when(even)
    def _():
        left_near()

    @pl.when(jnp.logical_and(odd, me != last))
    def _():
        right_near(False)

    def finish_rounds(far, late):
        if not late:
            arrive(copies[5])
            put_within(halo.at[5], x0.at[3, :, W])
        inside = square(x1[1]) if far else part_w0[...] + square(x1[1, :, A])
        _, new = keep(inside, x1[1, :, W])
        put_sum(4, new)
        x2[0, :, W] = new.astype(F8)
        _, new = keep(between(x1, 1), x1[1, :, A])
        put_sum(5, new)
        x2[0, :, A] = new.astype(F8)
        first = plain(x0[2, :, W], x0[2, :, A])
        if late:
            part_a0[...] = first
            part_w1[...] = square(x1[2, :, : 2 * t])
        else:
            _, new = keep(first + dot_nt(x0[2, :, A], x0[3, :, W]), x0[2, :, A])
            x1[2, :, A] = new.astype(F8)
        if far:
            left_far()
        if not late:
            _, new = keep(square(x1[2]), x1[2, :, W])
            x2[1, :, W] = new.astype(F8)
        support = square(x2[0]) if far else part_top[...] + square(x2[0, :, t:])
        _, new = keep(support, x2[0, :, W])
        put_sum(6, new)
        out_ref[:, :t] = support * new
        first = plain(x2[0, :, W], x2[0, :, A])
        if late:
            part_w0[...] = first
            arrive(copies[5])
            put_within(halo.at[5], x0.at[3, :, W])
            support = part_a0[...] + dot_nt(x0[2, :, A], x0[3, :, W])
            _, new = keep(support, x0[2, :, A])
            x1[2, :, A] = new.astype(F8)
            _, new = keep(part_w1[...] + square(x1[2, :, A]), x1[2, :, W])
            x2[1, :, W] = new.astype(F8)
            first = part_w0[...]
        support = first + dot_nt(x2[0, :, A], x2[1, :, W])
        _, new = keep(support, x2[0, :, A])
        put_sum(7, new)
        out_ref[:, t:] = support * new

    @pl.when(me == last)
    def _():
        finish_rounds(False, False)

    @pl.when(me == last - 1)
    def _():
        arrive(copies[0])
        finish_rounds(True, True)

    @pl.when(me < last - 1)
    def _():
        arrive(copies[0])
        finish_rounds(True, False)

    counts = []
    for step in range(ITERS):
        before, after = sums[2 * step : 2 * step + 2, :], sums[2 * step + 2 : 2 * step + 4, :]
        gone = before - after
        counts.append(gone[0:1] + 2.0 * gone[1:2])
    lane = lax.broadcasted_iota(jnp.int32, (1, 128), 1)
    packed = jnp.zeros((1, 128), F32)
    for step, row in enumerate(counts):
        packed = jnp.where(lane == step, jnp.sum(row, axis=1, keepdims=True), packed)
    mine[...] = packed.astype(jnp.int32)

    def share(d, carry):
        send(mine, gathered.at[d - 1], cnt_send, cnt_recv, lax.rem(me + d, n)).start()
        return carry

    @pl.when(me != root)
    def _():
        pl.semaphore_wait(all_in, 1)

    lax.fori_loop(1, n, share, 0)
    for slot in range(1, 5):
        left(copies[slot])

    @pl.when(even)
    def _():
        left(copies[0])
        left(to_right)

    @pl.when(odd)
    def _():
        left(copies[5])
        left(to_left)

    @pl.when(me == mid_next)
    def _():
        left(hop_out[3])
        left(hop_out[4])

    @pl.when(me == mid)
    def _():
        left(hop_out[5])

    pltpu.make_async_copy(gathered, gathered, cnt_recv).wait()
    cnt_ref[: n - 1] = gathered[...]
    cnt_ref[n - 1] = mine[...]
    pltpu.make_async_copy(gathered, gathered, cnt_send).wait()


def finish(support_ref, cnt_ref, out_ref, removed_ref, sems):
    parts = sems.shape[0]
    rows = support_ref.shape[0] // parts
    copies = [
        pltpu.make_async_copy(
            support_ref.at[pl.ds(i * rows, rows)], out_ref.at[pl.ds(i * rows, rows)], sems.at[i]
        )
        for i in range(parts)
    ]
    for copy in copies:
        copy.start()
    summed = jnp.sum(cnt_ref[...], axis=0)
    lane = lax.broadcasted_iota(jnp.int32, summed.shape, 1)
    for step in range(removed_ref.shape[0]):
        removed_ref[step] = jnp.sum(jnp.where(lane == step, summed, 0)) // 2
    for copy in copies:
        copy.wait()


def on_device(n, adj_diag, adj_right, alive_diag, alive_right, truss_k):
    words, t = adj_diag.shape
    vmem = pl.BlockSpec(memory_space=pltpu.VMEM)
    smem = pl.BlockSpec(memory_space=pltpu.SMEM)
    hbm = pl.BlockSpec(memory_space=pltpu.HBM)
    args = [
        pltpu.with_memory_space_constraint(v, pltpu.HBM)
        for v in (adj_diag, adj_right, alive_diag, alive_right)
    ]
    support, counts = pl.pallas_call(
        functools.partial(kernel, n),
        out_shape=(
            jax.ShapeDtypeStruct((t, 2 * t), F32),
            jax.ShapeDtypeStruct((n, 1, 128), jnp.int32),
        ),
        in_specs=[hbm] * 5,
        out_specs=(vmem, vmem),
        scratch_shapes=[
            pltpu.SMEM((1,), jnp.int32),
            pltpu.VMEM((4, words, t), jnp.int32),
            pltpu.VMEM((2, words, t), jnp.int32),
            pltpu.VMEM((6, words, t), jnp.int32),
            pltpu.VMEM((3, words, t), jnp.int32),
            pltpu.VMEM((4, t, 3 * t), F8),
            pltpu.VMEM((3, t, 3 * t), F8),
            pltpu.VMEM((2, t, 3 * t), F8),
            pltpu.VMEM((t // 2, t // 2), F8),
            pltpu.VMEM((t, t), F8),
            pltpu.VMEM((t, t), F8),
            pltpu.VMEM((8, 128), F32),
            pltpu.VMEM((1, 128), jnp.int32),
            pltpu.VMEM((n - 1, 1, 128), jnp.int32),
            *[pltpu.VMEM((t, t), F32)] * 4,
            pltpu.SemaphoreType.DMA,
            pltpu.SemaphoreType.DMA((4,)),
            pltpu.SemaphoreType.DMA((6, 2)),
            pltpu.SemaphoreType.DMA((12,)),
            pltpu.SemaphoreType.DMA((2,)),
            pltpu.SemaphoreType.DMA((3, 2)),
            pltpu.SemaphoreType.DMA((3, 2)),
            pltpu.SemaphoreType.DMA,
            pltpu.SemaphoreType.DMA,
            pltpu.SemaphoreType.REGULAR,
            pltpu.SemaphoreType.REGULAR,
        ],
        compiler_params=pltpu.CompilerParams(collective_id=0, has_side_effects=True, vmem_limit_bytes=32 * 2**20),
    )(truss_k, *args)
    return pl.pallas_call(
        finish,
        out_shape=(
            jax.ShapeDtypeStruct((t, 2 * t), F32),
            jax.ShapeDtypeStruct((ITERS,), jnp.int32),
        ),
        in_specs=[vmem, vmem],
        out_specs=(hbm, smem),
        scratch_shapes=[pltpu.SemaphoreType.DMA((4,))],
        compiler_params=pltpu.CompilerParams(vmem_limit_bytes=2**20),
    )(support, counts)


def solution(mesh):
    row = P("rows", None)
    return jax.shard_map(
        functools.partial(on_device, mesh.shape["rows"]),
        mesh=mesh,
        in_specs=(row, row, row, row, P()),
        out_specs=(row, P()),
        check_vma=False,
    )
```

```python
import functools

import jax
import jax.numpy as jnp
from jax import lax
from jax.experimental import pallas as pl
from jax.experimental.pallas import tpu as pltpu
from jax.sharding import PartitionSpec as P

F8 = jnp.float8_e4m3fn
F32 = jnp.float32
WORD = 32
ITERS = 3


def dot_nt(lhs, rhs):
    return lax.dot_general(lhs, rhs, (((1,), (1,)), ((), ())), preferred_element_type=F32)


def send(src, dst, send_sem, recv_sem, target):
    return pltpu.make_async_remote_copy(
        src_ref=src,
        dst_ref=dst,
        send_sem=send_sem,
        recv_sem=recv_sem,
        device_id=(target,),
        device_id_type=pl.DeviceIdType.MESH,
    )


def kernel(
    n, k_ref, ad_ref, ar_ref, ld_ref, lr_ref, out_ref, cnt_ref,
    k_smem, raw, own, halo, hop, x0, x1, x2, eye, tri, spare, sums, mine, gathered,
    part_w0, part_a0, part_w1, part_top,
    k_sem, raw_sems, send_sems, recv_sems, relay_sems, hop_send, hop_recv, cnt_send, cnt_recv,
    all_in, last_in, near_in,
):
    t = ad_ref.shape[1]
    words = ad_ref.shape[0]
    me = lax.axis_index("rows")
    even = lax.rem(me, 2) == 0
    barrier = pltpu.get_barrier_semaphore()

    odd = jnp.logical_not(even)
    last, mid, mid_next, root = n - 1, n // 2, n // 2 + 1, n - 5

    def greet(target):
        pl.semaphore_signal(
            barrier, inc=1, device_id=(target,), device_id_type=pl.DeviceIdType.MESH
        )

    def at(by):
        return lax.rem(me + by + n, n)

    greet(at(-1))

    @pl.when(me != last)
    def _():
        greet(at(1))

    @pl.when(even)
    def _():
        greet(at(-2))

    @pl.when(jnp.logical_and(odd, me != last))
    def _():
        greet(at(2))

    @pl.when(me == last)
    def _():
        greet(last - 2)

    @pl.when(me == mid)
    def _():
        greet(1)
        greet(last)

    @pl.when(me == mid_next)
    def _():
        greet(0)
        greet(last)
        greet(last - 1)

    @pl.when(jnp.logical_or(me < root - 2, me > root + 1))
    def _():
        greet(root)

    loads = [
        pltpu.make_async_copy(src, raw.at[i], raw_sems.at[i])
        for i, src in enumerate((ad_ref, ar_ref, ld_ref, lr_ref))
    ]
    for load in loads:
        load.start()
    k_load = pltpu.make_async_copy(k_ref, k_smem, k_sem)
    k_load.start()
    @pl.when(me == last)
    def _():
        pl.semaphore_wait(barrier, 5)
        for target in (mid, mid_next):
            pl.semaphore_signal(
                last_in, inc=1, device_id=(target,), device_id_type=pl.DeviceIdType.MESH
            )

    @pl.when(me == last - 1)
    def _():
        pl.semaphore_wait(barrier, 4)
        pl.semaphore_signal(
            near_in, inc=1, device_id=(mid_next,), device_id_type=pl.DeviceIdType.MESH
        )

    for load in loads:
        load.wait()
    own[0] = raw[0] & raw[2]
    own[1] = raw[1] & raw[3]

    AT, W, A = (pl.ds(i * t, t) for i in range(3))
    shift = lax.broadcasted_iota(jnp.int32, (WORD, t), 0)
    slope = lax.broadcasted_iota(jnp.int32, (WORD, 128), 1) - shift[:, :128]

    half = t // 2

    def bits_of(src, w, cols):
        span = cols.size
        words32 = jnp.broadcast_to(src[w : w + 1, cols], (WORD, span))
        return (words32 >> shift[:, :span]) & 1

    def put_across(src, dst):
        for w in range(words):
            dst[pl.ds(WORD * w, WORD), :] = bits_of(src, w, pl.ds(0, t)).astype(F32).astype(F8)

    halves = (pl.ds(0, half), pl.ds(half, half))

    def flipped(src, rows, cols):
        return dot_nt(eye[...], src[cols, rows])

    def put_flipped(src, dst):
        for rows in halves:
            for cols in halves:
                dst[rows, cols] = flipped(src, rows, cols).astype(F8)

    def put_within(src, dst):
        for w in range(words):
            rows, edge = pl.ds(WORD * w, WORD), WORD * w // 128 * 128
            bits = bits_of(src, w, pl.ds(edge, 128))
            bits = jnp.where(slope > WORD * w - edge, bits, 0)
            tri[rows, pl.ds(edge, 128)] = bits.astype(F32).astype(F8)
            if edge + 128 < t:
                rest = pl.ds(edge + 128, t - edge - 128)
                tri[rows, rest] = bits_of(src, w, rest).astype(F32).astype(F8)
        for rows in halves:
            both = flipped(tri, rows, rows) + tri[rows, rows].astype(F32)
            dst[rows, rows] = both.astype(F8)
        first, second = halves
        dst[first, second] = tri[first, second]
        dst[second, first] = flipped(tri, second, first).astype(F8)

    row_id = lax.broadcasted_iota(jnp.int32, (half, half), 0)
    col_id = lax.broadcasted_iota(jnp.int32, (half, half), 1)
    eye[...] = jnp.where(row_id == col_id, 1.0, 0.0).astype(F32).astype(F8)
    tri[...] = jnp.zeros((t, t), F32).astype(F8)

    @pl.when(me == root)
    def _():
        pl.semaphore_wait(barrier, n - 1)

    @pl.when(me == last - 2)
    def _():
        pl.semaphore_wait(barrier, 4)

    @pl.when(jnp.logical_and(me != root, me < last - 2))
    def _():
        pl.semaphore_wait(barrier, 3)

    top, low = pl.ds(0, words // 2), pl.ds(words // 2, words // 2)
    whole, right = pl.ds(0, t), pl.ds(half, half)

    def pieces(source, dest, upper, sends, recvs, target):
        parts = [(top, whole), (low, right if upper else whole)]
        return [
            send(
                source.at[rows, cols], dest.at[rows, cols], sends.at[i], recvs[i], target
            )
            for i, (rows, cols) in enumerate(parts)
        ]

    def to_halo(source, slot, sends, target):
        recvs = [recv_sems.at[2 * slot + i] for i in range(2)]
        return pieces(source, halo.at[slot], slot in (1, 3, 5), sends, recvs, target)

    def to_hop(what, place, slot, target):
        recvs = [hop_recv.at[place, i] for i in range(2)]
        return pieces(own.at[what], hop.at[place], slot in (3, 5), send_sems.at[slot], recvs, target)

    def start(pieces):
        for piece in pieces:
            piece.start()

    def arrive(pieces):
        for piece in pieces:
            piece.wait_recv()

    def left(pieces):
        for piece in pieces:
            piece.wait_send()

    routes = {2: (1, 1), 3: (0, -1), 1: (0, 1), 4: (1, -1), 0: (1, 2), 5: (0, -2)}
    copies = {
        slot: to_halo(own.at[what], slot, send_sems.at[slot], at(by))
        for slot, (what, by) in routes.items()
    }
    to_right = to_halo(halo.at[2], 0, relay_sems, at(1))
    to_left = to_halo(halo.at[3], 5, relay_sems, at(-1))
    hop_in = {3: to_hop(0, 0, 3, mid_next), 4: to_hop(1, 1, 4, mid_next), 5: to_hop(0, 2, 5, mid)}
    hop_out = {
        slot: to_halo(hop.at[slot - 3], slot, hop_send.at[slot - 3], last) for slot in (3, 4, 5)
    }

    def start_or_hop(slot, source):
        @pl.when(me == source)
        def _():
            start(hop_in[slot])

        @pl.when(me != source)
        def _():
            start(copies[slot])

    direct = to_halo(own.at[1], 0, hop_send.at[0], last)
    hop_near = to_halo(hop.at[0], 5, hop_send.at[2], last - 1)
    start_or_hop(3, 0)
    start(copies[2])

    start_or_hop(4, 0)
    start(copies[1])

    @pl.when(me == last - 2)
    def _():
        start(direct)

    @pl.when(me == 1)
    def _():
        start(hop_in[5])

    @pl.when(me == root)
    def _():
        def tell(d, carry):
            pl.semaphore_signal(
                all_in, inc=1, device_id=(at(d),), device_id_type=pl.DeviceIdType.MESH
            )
            return carry

        lax.fori_loop(1, n, tell, 0)

    def total(values):
        lanes = jnp.sum(values, axis=0, keepdims=True)
        return sum(lanes[:, i : i + 128] for i in range(0, t, 128))

    def keep(support, ref):
        old = ref.astype(F32)
        return old, jnp.where(support >= thresh, old, 0.0)

    def put_sum(row, values):
        sums[row : row + 1, :] = total(values)

    def plain(lhs, rhs):
        return jnp.dot(lhs, rhs, preferred_element_type=F32)

    def square(block):
        return dot_nt(block, block)

    def between(x, j):
        return dot_nt(x[j, :, t:], x[j + 1, :, : 2 * t])

    put_across(own.at[1], x0.at[1, :, A])
    k_load.wait()
    thresh = (k_smem[0] - 2).astype(F32)
    put_within(own.at[0], x0.at[1, :, W])
    put_flipped(x0.at[1, :, A], x0.at[2, :, AT])
    part_w0[...] = square(x0[1, :, t:])
    part_w1[...] = square(x0[2, :, AT])
    part_a0[...] = dot_nt(x0[1, :, W], x0[2, :, AT])

    @pl.when(even)
    def _():
        start(copies[0])

    @pl.when(jnp.logical_and(odd, me != 1))
    def _():
        start(copies[5])

    def pass_right():
        arrive(copies[2])
        start(to_right)

    def left_near():
        arrive(copies[1])
        put_across(halo.at[2], x0.at[0, :, A])
        put_flipped(x0.at[0, :, A], x0.at[1, :, AT])
        old, new = keep(part_w0[...] + square(x0[1, :, AT]), x0[1, :, W])
        put_sum(0, old)
        put_sum(2, new)
        x1[1, :, W] = new.astype(F8)
        put_within(halo.at[1], x0.at[0, :, W])
        _, new = keep(between(x0, 0), x0[0, :, A])
        x1[0, :, A] = new.astype(F8)
        put_flipped(x1.at[0, :, A], x1.at[1, :, AT])

    def left_far(early):
        put_across(halo.at[0], spare)
        put_flipped(spare, x0.at[0, :, AT])
        inside = part_top[...] + square(x0[0, :, AT]) if early else square(x0[0])
        _, new = keep(inside, x0[0, :, W])
        x1[0, :, W] = new.astype(F8)
        _, new = keep(between(x1, 0), x1[0, :, A])
        spare[...] = new.astype(F8)
        put_flipped(spare, x2.at[0, :, AT])

    def right_near(split):
        arrive(copies[3])

        @pl.when(jnp.logical_and(odd, me != last))
        def _():
            start(to_left)

        if not split:
            arrive(copies[4])
        put_within(halo.at[3], x0.at[2, :, W])
        old, new = keep(part_a0[...] + dot_nt(x0[1, :, A], x0[2, :, W]), x0[1, :, A])
        put_sum(1, old)
        put_sum(3, new)
        x1[1, :, A] = new.astype(F8)
        put_flipped(x1.at[1, :, A], x1.at[2, :, AT])
        if split:
            arrive(copies[4])
        put_across(halo.at[4], x0.at[2, :, A])
        _, new = keep(part_w1[...] + square(x0[2, :, t:]), x0[2, :, W])
        x1[2, :, W] = new.astype(F8)

    @pl.when(me == mid_next)
    def _():
        pl.semaphore_wait(last_in, 1)
        for slot in (3, 4):
            arrive(hop_in[slot])
            start(hop_out[slot])
        pl.semaphore_wait(near_in, 1)
        start(hop_near)

    @pl.when(odd)
    def _():
        arrive(copies[2])
        left_near()

    @pl.when(even)
    def _():
        right_near(False)

    @pl.when(me == mid)
    def _():
        pl.semaphore_wait(last_in, 1)
        arrive(hop_in[5])
        start(hop_out[5])

    @pl.when(me == last)
    def _():
        part_top[...] = square(x0[0, :, t:])
        part_w0[...] = square(x1[1, :, : 2 * t])
        arrive(copies[0])
        left_far(True)
        part_top[...] = square(x2[0, :, AT])
        right_near(True)

    @pl.when(jnp.logical_and(even, me != last - 1))
    def _():
        pass_right()

    @pl.when(me == last - 1)
    def _():
        arrive(copies[2])

    @pl.when(even)
    def _():
        left_near()

    @pl.when(jnp.logical_and(odd, me != last))
    def _():
        right_near(False)

    def finish_rounds(far, late):
        if not late:
            arrive(copies[5])
            put_within(halo.at[5], x0.at[3, :, W])
        inside = square(x1[1]) if far else part_w0[...] + square(x1[1, :, A])
        _, new = keep(inside, x1[1, :, W])
        put_sum(4, new)
        x2[0, :, W] = new.astype(F8)
        _, new = keep(between(x1, 1), x1[1, :, A])
        put_sum(5, new)
        x2[0, :, A] = new.astype(F8)
        first = plain(x0[2, :, W], x0[2, :, A])
        if late:
            part_a0[...] = first
            part_w1[...] = square(x1[2, :, : 2 * t])
        else:
            _, new = keep(first + dot_nt(x0[2, :, A], x0[3, :, W]), x0[2, :, A])
            x1[2, :, A] = new.astype(F8)
        if far:
            left_far(False)
        if not late:
            _, new = keep(square(x1[2]), x1[2, :, W])
            x2[1, :, W] = new.astype(F8)
        support = square(x2[0]) if far else part_top[...] + square(x2[0, :, t:])
        _, new = keep(support, x2[0, :, W])
        put_sum(6, new)
        out_ref[:, :t] = support * new
        first = plain(x2[0, :, W], x2[0, :, A])
        if late:
            part_w0[...] = first
            arrive(copies[5])
            put_within(halo.at[5], x0.at[3, :, W])
            support = part_a0[...] + dot_nt(x0[2, :, A], x0[3, :, W])
            _, new = keep(support, x0[2, :, A])
            x1[2, :, A] = new.astype(F8)
            _, new = keep(part_w1[...] + square(x1[2, :, A]), x1[2, :, W])
            x2[1, :, W] = new.astype(F8)
            first = part_w0[...]
        support = first + dot_nt(x2[0, :, A], x2[1, :, W])
        _, new = keep(support, x2[0, :, A])
        put_sum(7, new)
        out_ref[:, t:] = support * new

    @pl.when(me == last)
    def _():
        finish_rounds(False, False)

    @pl.when(me == last - 1)
    def _():
        arrive(copies[0])
        finish_rounds(True, True)

    @pl.when(me < last - 1)
    def _():
        arrive(copies[0])
        finish_rounds(True, False)

    counts = []
    for step in range(ITERS):
        before, after = sums[2 * step : 2 * step + 2, :], sums[2 * step + 2 : 2 * step + 4, :]
        gone = before - after
        counts.append(gone[0:1] + 2.0 * gone[1:2])
    lane = lax.broadcasted_iota(jnp.int32, (1, 128), 1)
    packed = jnp.zeros((1, 128), F32)
    for step, row in enumerate(counts):
        packed = jnp.where(lane == step, jnp.sum(row, axis=1, keepdims=True), packed)
    mine[...] = packed.astype(jnp.int32)

    def share(d, carry):
        send(mine, gathered.at[d - 1], cnt_send, cnt_recv, lax.rem(me + d, n)).start()
        return carry

    @pl.when(me != root)
    def _():
        pl.semaphore_wait(all_in, 1)

    lax.fori_loop(1, n, share, 0)
    for slot in range(1, 5):
        left(copies[slot])

    @pl.when(even)
    def _():
        left(copies[0])

    @pl.when(jnp.logical_and(even, me != last - 1))
    def _():
        left(to_right)

    @pl.when(me == last - 2)
    def _():
        left(direct)

    @pl.when(odd)
    def _():
        left(copies[5])

    @pl.when(jnp.logical_and(odd, me != last))
    def _():
        left(to_left)

    @pl.when(me == mid_next)
    def _():
        left(hop_out[3])
        left(hop_out[4])
        left(hop_near)

    @pl.when(me == mid)
    def _():
        left(hop_out[5])

    pltpu.make_async_copy(gathered, gathered, cnt_recv).wait()
    cnt_ref[: n - 1] = gathered[...]
    cnt_ref[n - 1] = mine[...]
    pltpu.make_async_copy(gathered, gathered, cnt_send).wait()


def finish(support_ref, cnt_ref, out_ref, removed_ref, sems):
    parts = sems.shape[0]
    rows = support_ref.shape[0] // parts
    copies = [
        pltpu.make_async_copy(
            support_ref.at[pl.ds(i * rows, rows)], out_ref.at[pl.ds(i * rows, rows)], sems.at[i]
        )
        for i in range(parts)
    ]
    for copy in copies:
        copy.start()
    summed = jnp.sum(cnt_ref[...], axis=0)
    lane = lax.broadcasted_iota(jnp.int32, summed.shape, 1)
    for step in range(removed_ref.shape[0]):
        removed_ref[step] = jnp.sum(jnp.where(lane == step, summed, 0)) // 2
    for copy in copies:
        copy.wait()


def on_device(n, adj_diag, adj_right, alive_diag, alive_right, truss_k):
    words, t = adj_diag.shape
    vmem = pl.BlockSpec(memory_space=pltpu.VMEM)
    smem = pl.BlockSpec(memory_space=pltpu.SMEM)
    hbm = pl.BlockSpec(memory_space=pltpu.HBM)
    args = [
        pltpu.with_memory_space_constraint(v, pltpu.HBM)
        for v in (adj_diag, adj_right, alive_diag, alive_right)
    ]
    support, counts = pl.pallas_call(
        functools.partial(kernel, n),
        out_shape=(
            jax.ShapeDtypeStruct((t, 2 * t), F32),
            jax.ShapeDtypeStruct((n, 1, 128), jnp.int32),
        ),
        in_specs=[hbm] * 5,
        out_specs=(vmem, vmem),
        scratch_shapes=[
            pltpu.SMEM((1,), jnp.int32),
            pltpu.VMEM((4, words, t), jnp.int32),
            pltpu.VMEM((2, words, t), jnp.int32),
            pltpu.VMEM((6, words, t), jnp.int32),
            pltpu.VMEM((3, words, t), jnp.int32),
            pltpu.VMEM((4, t, 3 * t), F8),
            pltpu.VMEM((3, t, 3 * t), F8),
            pltpu.VMEM((2, t, 3 * t), F8),
            pltpu.VMEM((t // 2, t // 2), F8),
            pltpu.VMEM((t, t), F8),
            pltpu.VMEM((t, t), F8),
            pltpu.VMEM((8, 128), F32),
            pltpu.VMEM((1, 128), jnp.int32),
            pltpu.VMEM((n - 1, 1, 128), jnp.int32),
            *[pltpu.VMEM((t, t), F32)] * 4,
            pltpu.SemaphoreType.DMA,
            pltpu.SemaphoreType.DMA((4,)),
            pltpu.SemaphoreType.DMA((6, 2)),
            pltpu.SemaphoreType.DMA((12,)),
            pltpu.SemaphoreType.DMA((2,)),
            pltpu.SemaphoreType.DMA((3, 2)),
            pltpu.SemaphoreType.DMA((3, 2)),
            pltpu.SemaphoreType.DMA,
            pltpu.SemaphoreType.DMA,
            pltpu.SemaphoreType.REGULAR,
            pltpu.SemaphoreType.REGULAR,
            pltpu.SemaphoreType.REGULAR,
        ],
        compiler_params=pltpu.CompilerParams(collective_id=0, has_side_effects=True, vmem_limit_bytes=32 * 2**20),
    )(truss_k, *args)
    return pl.pallas_call(
        finish,
        out_shape=(
            jax.ShapeDtypeStruct((t, 2 * t), F32),
            jax.ShapeDtypeStruct((ITERS,), jnp.int32),
        ),
        in_specs=[vmem, vmem],
        out_specs=(hbm, smem),
        scratch_shapes=[pltpu.SemaphoreType.DMA((4,))],
        compiler_params=pltpu.CompilerParams(vmem_limit_bytes=2**20),
    )(support, counts)


def solution(mesh):
    row = P("rows", None)
    return jax.shard_map(
        functools.partial(on_device, mesh.shape["rows"]),
        mesh=mesh,
        in_specs=(row, row, row, row, P()),
        out_specs=(row, P()),
        check_vma=False,
    )
```
